32 devices in a mesh: dp: 8 (over z, x), mp: 4 (over y, core).
Axes of the slice: x: 2, y: 2, z: 4, core: 2. Of those that a mesh axis runs over, the one named last changes fastest.
Arguments:
- gradients: bfloat16 [8, 3584, 14336], P(None, 'dp', 'mp'), may hold values from -60 to 60
- column_slot: int32 [8, 16], replicated, may hold values from 0 to 31, as said below
- left_roots: bfloat16 [32, 4, 4, 896, 896], P('dp', 'mp'), may hold values from -1 to 5
- right_roots: bfloat16 [32, 4, 4, 896, 896], P('dp', 'mp'), may hold values from -1 to 5
Outputs:
- update: bfloat16 [8, 3584, 14336], P(None, 'dp', 'mp')
- clip_scale: float32 [], replicated
The draws below stay inside these ranges and needn't reach their ends.
Inputs may be any that keep to these rules, and one draw needn't show every extreme that they name: `column_slot`: block column c belongs to group c // 4; over all matrices, the entries of one group's block columns are a permutation of 0 to 31.
All inputs are finite; a program needn't handle non-finite values.
Results may differ from the reference program's by a relative error of at most 0.0049.
Values may be sent and summed in bfloat16 or wider, within the bound.
A program may use at most 256 MiB of HBM per device.

```python
import math
import jax
import jax.numpy as jnp
from jax import lax

D = 3584
FF = 14336
BLOCK = 896
MATRICES = 8
ROW_BLOCKS = 4
COLUMNS = 16
COLS_MP = 4
SLOTS = 32
N_MP = 4


def draw_gradients(key, part):
    keys = jax.random.split(jax.random.fold_in(key, 5), 3)
    ramp = jnp.sqrt(1.0 + 2.0 * jnp.arange(D, dtype=jnp.float32) / (D - 1)).reshape(1, D, 1)
    col_scale = jnp.exp(jax.random.uniform(keys[1], (MATRICES, 1, FF), jnp.float32, 0.0, math.log(10.0)))
    row_scale = jnp.exp(jax.random.uniform(keys[0], (MATRICES, D, 1), jnp.float32, 0.0, math.log(10.0)))
    base = jnp.clip(jax.random.normal(keys[2], (MATRICES, D, FF), jnp.float32), -6.0, 6.0)
    values = base * row_scale * col_scale * ramp / 21.5
    return jnp.clip(values, -60.0, 60.0).astype(jnp.bfloat16)


def draw_column_slot(key, part):
    keys = jax.random.split(jax.random.fold_in(key, 11), N_MP)

    def permute_one(sub_key):
        return jax.random.permutation(sub_key, SLOTS)
    perms = jax.vmap(permute_one)(keys).astype(jnp.int32)
    table = perms.reshape(N_MP, MATRICES, COLS_MP).transpose(1, 0, 2).reshape(MATRICES, COLUMNS)
    return table.astype(jnp.int32)


def draw_roots(key):
    keys = jax.random.split(key, 2)
    shape = (SLOTS, N_MP, ROW_BLOCKS, BLOCK, BLOCK)
    noise = jnp.clip(jax.random.normal(keys[0], shape, jnp.float32), -4.0, 4.0)
    symmetric = (noise + jnp.swapaxes(noise, -1, -2)) * (0.35 / math.sqrt(2.0 * BLOCK))
    diagonal = jnp.exp(jax.random.uniform(keys[1], shape[:-1], jnp.float32, math.log(0.5), math.log(2.0)))
    matrix = symmetric + diagonal[..., None] * jnp.eye(BLOCK, dtype=jnp.float32)
    return matrix.astype(jnp.bfloat16)


def draw_left_roots(key, part):
    return draw_roots(jax.random.fold_in(key, 21))


def draw_right_roots(key, part):
    return draw_roots(jax.random.fold_in(key, 37))


def setup_inputs(seed: int = 0) -> dict:
    splits = jax.random.split(jax.random.key(seed), 5)
    gradients = draw_gradients(jax.random.fold_in(splits[4], 71), 0)
    column_slot = draw_column_slot(jax.random.fold_in(splits[4], 71), 0)
    left_roots = draw_left_roots(jax.random.fold_in(splits[4], 71), 0)
    right_roots = draw_right_roots(jax.random.fold_in(splits[4], 71), 0)
    return {"gradients": gradients, "column_slot": column_slot, "left_roots": left_roots, "right_roots": right_roots}


rms_limit = 0.25
epsilon = 1e-06

def reference(gradients, column_slot, left_roots, right_roots):
    widened = gradients.astype(jnp.float32)
    square_sum = jnp.sum(widened * widened)
    mean_square = square_sum / (MATRICES * D * FF)
    clip_scale = jnp.minimum(jnp.float32(1.0), rms_limit / jnp.sqrt(mean_square + epsilon)).astype(jnp.float32)
    zero_index = jnp.zeros((), jnp.int32)

    def one_column(flat_index):
        matrix = (flat_index // COLUMNS).astype(jnp.int32)
        block_col = (flat_index % COLUMNS).astype(jnp.int32)
        group_index = (block_col // COLS_MP).astype(jnp.int32)
        slot_index = column_slot[matrix, block_col].astype(jnp.int32)
        block_grad = lax.dynamic_slice(gradients, (matrix, zero_index, (block_col * BLOCK).astype(jnp.int32)), (1, D, BLOCK))
        block_grad = block_grad.reshape(ROW_BLOCKS, BLOCK, BLOCK).astype(jnp.float32)
        starts = (slot_index, group_index, zero_index, zero_index, zero_index)
        left_root = lax.dynamic_slice(left_roots, starts, (1, 1, ROW_BLOCKS, BLOCK, BLOCK)).reshape(ROW_BLOCKS, BLOCK, BLOCK)
        right_root = lax.dynamic_slice(right_roots, starts, (1, 1, ROW_BLOCKS, BLOCK, BLOCK)).reshape(ROW_BLOCKS, BLOCK, BLOCK)
        first_product = jnp.einsum('nab,nbc->nac', left_root.astype(jnp.float32), block_grad)
        scaled = (clip_scale * first_product).astype(jnp.bfloat16)
        second_product = jnp.einsum('nab,nbc->nac', scaled.astype(jnp.float32), right_root.astype(jnp.float32))
        return second_product.astype(jnp.bfloat16).reshape(D, BLOCK)
    columns = lax.map(one_column, jnp.arange(MATRICES * COLUMNS, dtype=jnp.int32))
    update = columns.reshape(MATRICES, COLUMNS, D, BLOCK).transpose(0, 2, 1, 3).reshape(MATRICES, D, FF)
    return (update, clip_scale)
```

```python
import functools
import math

import jax
import jax.numpy as jnp
from jax import lax
from jax.experimental import pallas as pl
from jax.experimental.pallas import tpu as pltpu
from jax.sharding import PartitionSpec as P

rms_limit = 0.25
epsilon = 1e-06
VMEM_LIMIT = 48 * 1024 * 1024


def pack_kernel(matrix_ref, column_ref, x_ref, o_ref, s_ref):
    @pl.when(pl.program_id(0) == 0)
    def _():
        s_ref[...] = jnp.zeros_like(s_ref)

    x = x_ref[0]
    o_ref[0] = x
    wide = x.astype(jnp.float32)
    s_ref[...] += jnp.sum((wide * wide).reshape(-1, 8, wide.shape[-1]), axis=0)


def pack(gradients, matrix_of, column_of, block):
    count = matrix_of.shape[0]
    rows = gradients.shape[1]
    spec = pltpu.PrefetchScalarGridSpec(
        num_scalar_prefetch=2,
        grid=(count,),
        in_specs=[pl.BlockSpec((1, rows, block), lambda i, m, c: (m[i], 0, c[i]))],
        out_specs=[
            pl.BlockSpec((1, rows, block), lambda i, m, c: (i, 0, 0)),
            pl.BlockSpec((8, block), lambda i, m, c: (0, 0)),
        ],
    )
    size = count * rows * block
    return pl.pallas_call(
        pack_kernel,
        grid_spec=spec,
        out_shape=[
            jax.ShapeDtypeStruct((count, rows, block), gradients.dtype),
            jax.ShapeDtypeStruct((8, block), jnp.float32),
        ],
        cost_estimate=pl.CostEstimate(
            flops=2 * size, bytes_accessed=4 * size, transcendentals=0
        ),
    )(matrix_of, column_of, gradients)


def product_kernel(clip_ref, x_ref, l_ref, r_ref, o_ref):
    block = l_ref.shape[-1]
    x = x_ref[...].reshape(block, block)
    first = jnp.dot(l_ref[0, 0, 0], x, preferred_element_type=jnp.float32)
    scaled = (clip_ref[0] * first).astype(jnp.bfloat16)
    second = jnp.dot(scaled, r_ref[0, 0, 0], preferred_element_type=jnp.float32)
    o_ref[...] = second.astype(o_ref.dtype).reshape(o_ref.shape)


def products(clip, received, left_roots, right_roots, first_slot):
    peers, slots, rows, block = received.shape
    row_blocks = left_roots.shape[2]
    per_block = block // rows
    root_spec = pl.BlockSpec(
        (1, 1, 1, block, block), lambda s, r: (first_slot + s, 0, r, 0, 0)
    )
    block_spec = pl.BlockSpec((per_block, 1, rows, block), lambda s, r: (r, s, 0, 0))
    count = slots * row_blocks
    return pl.pallas_call(
        product_kernel,
        grid=(slots, row_blocks),
        in_specs=[
            pl.BlockSpec(memory_space=pltpu.SMEM),
            block_spec,
            root_spec,
            root_spec,
        ],
        out_specs=block_spec,
        out_shape=jax.ShapeDtypeStruct(received.shape, received.dtype),
        compiler_params=pltpu.CompilerParams(vmem_limit_bytes=VMEM_LIMIT),
        cost_estimate=pl.CostEstimate(
            flops=4 * count * block**3,
            bytes_accessed=8 * count * block**2,
            transcendentals=0,
        ),
    )(clip, received, left_roots, right_roots)


def unpack_kernel(matrix_ref, column_ref, x_ref, *refs):
    refs[-1][0] = x_ref[0]


def unpack(returned, matrix_of, column_of, shape, partial):
    count, rows, block = returned.shape
    in_specs = [pl.BlockSpec((1, rows, block), lambda i, m, c: (i, 0, 0))]
    operands = [matrix_of, column_of, returned]
    aliases = {}
    if partial is not None:
        in_specs.append(pl.BlockSpec(memory_space=pl.ANY))
        operands.append(partial)
        aliases = {3: 0}
    spec = pltpu.PrefetchScalarGridSpec(
        num_scalar_prefetch=2,
        grid=(count,),
        in_specs=in_specs,
        out_specs=pl.BlockSpec((1, rows, block), lambda i, m, c: (m[i], 0, c[i])),
    )
    size = count * rows * block
    return pl.pallas_call(
        unpack_kernel,
        grid_spec=spec,
        out_shape=jax.ShapeDtypeStruct(shape, returned.dtype),
        input_output_aliases=aliases,
        cost_estimate=pl.CostEstimate(
            flops=0, bytes_accessed=4 * size, transcendentals=0
        ),
    )(*operands)


def body(peers, total, gradients, column_slot, left_roots, right_roots):
    matrices, rows, width = gradients.shape
    owned, block = left_roots.shape[0], left_roots.shape[-1]
    local_cols = width // block
    chunks = 2 if owned % 2 == 0 else 1
    per = owned // chunks
    slot_count = matrices * local_cols
    mp_index = lax.axis_index("mp")
    my_slots = lax.dynamic_slice_in_dim(
        column_slot, mp_index * local_cols, local_cols, 1
    ).reshape(slot_count)
    ids = jnp.arange(slot_count, dtype=jnp.int32)
    order = jnp.sum(jnp.where(my_slots[None, :] == ids[:, None], ids[None, :], 0), axis=1)
    order = order.astype(jnp.int32).reshape(peers, chunks, per)
    matrix_of = [(order[:, k] // local_cols).reshape(-1) for k in range(chunks)]
    column_of = [(order[:, k] % local_cols).reshape(-1) for k in range(chunks)]

    packed, sums = [], []
    for k in range(chunks):
        chunk, partial = pack(gradients, matrix_of[k], column_of[k], block)
        packed.append(chunk)
        sums.append(partial)
    square_sum = lax.psum(jnp.sum(functools.reduce(jnp.add, sums)), ("dp", "mp"))
    clip_scale = jnp.minimum(
        jnp.float32(1.0), rms_limit / jnp.sqrt(square_sum / total + epsilon)
    )
    clip_scale, *packed = lax.optimization_barrier((clip_scale, *packed))
    clip = clip_scale.reshape(1)
    exchange = functools.partial(
        lax.all_to_all, axis_name="dp", split_axis=0, concat_axis=0, tiled=True
    )
    received = [exchange(c) for c in packed]
    returned = []
    for k in range(chunks):
        grid = received[k].reshape(peers, per, rows, block)
        finished = products(clip, grid, left_roots, right_roots, k * per)
        returned.append(exchange(finished.reshape(peers * per, rows, block)))
    update = None
    for k in range(chunks):
        update = unpack(returned[k], matrix_of[k], column_of[k], gradients.shape, update)
    return (update, clip_scale)


def solution(mesh):
    def run(gradients, column_slot, left_roots, right_roots):
        mapped = jax.shard_map(
            functools.partial(body, mesh.shape["dp"], math.prod(gradients.shape)),
            mesh=mesh,
            in_specs=(
                P(None, "dp", "mp"),
                P(),
                P("dp", "mp", None, None, None),
                P("dp", "mp", None, None, None),
            ),
            out_specs=(P(None, "dp", "mp"), P()),
            check_vma=False,
        )
        return mapped(gradients, column_slot, left_roots, right_roots)

    return run
```
